32 devices in a mesh: traj: 4 (over y, x), grid: 8 (over z, core).
Axes of the slice: x: 2, y: 2, z: 4, core: 2. Of those that a mesh axis runs over, the one named last changes fastest.
Arguments:
- psi_modes: float32 [4, 2, 256, 256, 256], P('traj', None, None, 'grid'), may hold values from -6 to 6
- noise: float32 [4, 2, 256, 256, 256], P('traj', None, 'grid'), may hold values from -6 to 6
- mask: int32 [256, 256, 256], P(None, 'grid'), may hold values from 0 to 1, as said below
Outputs:
- psi_next: float32 [4, 2, 256, 256, 256], P('traj', None, None, 'grid')
- momentum_hist: float32 [128], replicated
The draws below stay inside these ranges and needn't reach their ends.
Inputs may be any that keep to these rules, and one draw needn't show every extreme that they name: mask is 0 at every mode whose signed third index has magnitude 256/4 or more, and 1 at some mode whose signed third index has magnitude 256/4 - 1.
All inputs are finite; a program needn't handle non-finite values.
Results may differ from the reference program's by a relative error of at most 0.00023.
Values sent between devices are 32-bit elements; how exact they have to be, the bound alone decides.
A program may use at most 192 MiB of HBM per device.

```python
import jax
import jax.numpy as jnp
from jax import lax

NX = 256
NY = 256
NZ = 256
SHELLS = 128
TRAJ = 4


def signed_range(count):
    index = jnp.arange(count, dtype=jnp.int32)
    return jnp.where(index < count // 2, index, index - count)


def draw_mask(key, part):
    first, second = jax.random.split(jax.random.fold_in(key, 7))
    quarter = NZ // 4
    limit_sq = jax.random.randint(first, (), (quarter - 1) * (quarter - 1), 2 * (quarter - 1) * (quarter - 1) + 1)
    mode_x = signed_range(NX)[:, None, None]
    mode_y = signed_range(NY)[None, :, None]
    mode_z = signed_range(NZ)[None, None, :]
    radius_sq = mode_x * mode_x + mode_y * mode_y + mode_z * mode_z
    holes = jax.random.randint(second, (NX, NY, NZ), 0, 8) > 0
    anchor = (mode_x == 0) & (mode_y == 0)
    inside = (radius_sq <= limit_sq) & (jnp.abs(mode_z) < quarter) & (holes | anchor)
    return jnp.where(inside, 1, 0).astype(jnp.int32)


def shard_levels(rng, shape, cuts, smallest, high):
    factor_of, own = 1.0, jax.random.fold_in(rng, 6)
    for position, shards_of in cuts:
        heights = jnp.exp(jax.random.uniform(jax.random.fold_in(own, position), (shards_of,), jnp.float32, smallest / len(cuts), high / len(cuts)))
        factor_of = factor_of * jnp.repeat(heights, shape[position] // shards_of).reshape([-1 if axis == position else 1 for axis in range(len(shape))])
    return factor_of


def normal_values(key, extent, deviation, most, shards=(), kind=jnp.bfloat16):
    gain = shard_levels(key, extent, shards, -0.22, 0.18) if shards else 1.0
    result = jax.random.normal(key, extent, jnp.float32) * deviation * gain
    return jnp.minimum(jnp.maximum(result, -most), most).astype(kind)


def setup_inputs(seed: int = 0) -> dict:
    key_list = jax.random.split(jax.random.key(seed), 4)
    psi_modes = normal_values(key_list[0], (TRAJ, 2, NX, NY, NZ), 1.0, 6.0, ((0, 4), (3, 8)), jnp.float32)
    noise = normal_values(key_list[1], (TRAJ, 2, NX, NY, NZ), 1.0, 6.0, ((0, 4), (2, 8)), jnp.float32)
    mask = draw_mask(jax.random.fold_in(key_list[3], 71), 0)
    return dict(psi_modes=psi_modes, noise=noise, mask=mask)


time_step = 1.0
damping = 0.05
coupling = 10.0
chem_potential = 1.0
noise_amp = 0.1
trap_strength = 8.0


def signed_modes(count):
    index = jnp.arange(count, dtype=jnp.int32)
    return jnp.where(index < count // 2, index, index - count)


def wave_numbers(count):
    return signed_modes(count).astype(jnp.float32) * (2.0 * jnp.pi / count)


def positions(count):
    return (jnp.arange(count, dtype=jnp.float32) + 0.5) / count - 0.5


def reference(psi_modes, noise, mask):
    wave_x = wave_numbers(NX)
    wave_y = wave_numbers(NY)
    wave_z = wave_numbers(NZ)
    ksq = wave_x[:, None, None] ** 2 + wave_y[None, :, None] ** 2 + wave_z[None, None, :] ** 2
    theta = 0.25 * time_step * ksq
    magnitude = jnp.exp(-damping * theta) * mask.astype(jnp.float32)
    factor = lax.complex(magnitude * jnp.cos(theta), -magnitude * jnp.sin(theta))
    sig_x = signed_modes(NX)
    sig_y = signed_modes(NY)
    sig_z = signed_modes(NZ)
    radius_sq = sig_x[:, None, None] ** 2 + sig_y[None, :, None] ** 2 + sig_z[None, None, :] ** 2
    shells = jnp.minimum(radius_sq * SHELLS // (2 * (NZ // 4) * (NZ // 4)), SHELLS - 1).astype(jnp.int32)
    pos_x = positions(NX)
    pos_y = positions(NY)
    pos_z = positions(NZ)
    potential = trap_strength * (pos_x[:, None, None] ** 2 + pos_y[None, :, None] ** 2 + pos_z[None, None, :] ** 2)

    def per_traj(inputs):
        modes, forcing = inputs
        start = lax.complex(modes[0], modes[1]) * factor
        field = jnp.fft.ifftn(start, norm="ortho")
        density = jnp.real(field) ** 2 + jnp.imag(field) ** 2
        energy = potential + coupling * density - chem_potential
        decay = jnp.exp(-damping * energy * time_step)
        evolve = lax.complex(decay * jnp.cos(energy * time_step), -decay * jnp.sin(energy * time_step))
        moved = field * evolve + noise_amp * lax.complex(forcing[0], forcing[1])
        final = jnp.fft.fftn(moved, norm="ortho") * factor
        occupation = jnp.real(final) ** 2 + jnp.imag(final) ** 2
        partial_hist = jax.ops.segment_sum(occupation.reshape(-1), shells.reshape(-1), num_segments=SHELLS)
        return jnp.stack([jnp.real(final), jnp.imag(final)]), partial_hist

    results, partials = lax.map(per_traj, (psi_modes, noise))
    momentum_hist = jnp.sum(partials, axis=0) * (SHELLS / (TRAJ * NX * NY * NZ))
    return results, momentum_hist
```

```python
import jax
import jax.numpy as jnp
from jax import lax
from jax.sharding import PartitionSpec as P

SHELLS = 128


time_step = 1.0
damping = 0.05
coupling = 10.0
chem_potential = 1.0
noise_amp = 0.1
trap_strength = 8.0
max_chunks = 4


def signed_of(index, count):
    return jnp.where(index < count // 2, index, index - count)


def dft_table(out_index, in_index, count, sign):
    phase = (out_index[:, None] * in_index[None, :] % count).astype(jnp.float32) * (
        2.0 * jnp.pi / count
    )
    scale = 1.0 / jnp.sqrt(jnp.float32(count))
    return (jnp.cos(phase) * scale, sign * jnp.sin(phase) * scale)


def axis_factor(modes, count):
    wave = modes.astype(jnp.float32) * (2.0 * jnp.pi / count)
    theta = 0.25 * time_step * wave * wave
    size = jnp.exp(-damping * theta)
    return (size * jnp.cos(theta), -size * jnp.sin(theta))


def scaled(table, factor, dim):
    real, imag = factor
    if dim == 0:
        real, imag = real[:, None], imag[:, None]
    else:
        real, imag = real[None, :], imag[None, :]
    return (table[0] * real - table[1] * imag, table[0] * imag + table[1] * real)


def block_table(table):
    real, imag = table
    top = jnp.stack([real, -imag], axis=1)
    bottom = jnp.stack([imag, real], axis=1)
    return jnp.stack([top, bottom], axis=0)


def contract(pattern, table, values):
    return jnp.einsum(pattern, table, values, precision=lax.Precision.HIGH)


def cos_sin(angle):
    turns = jnp.round(angle * (2.0 / jnp.pi))
    rest = angle - turns * 1.5703125
    rest = rest - turns * 4.837512969970703125e-4
    rest = rest - turns * 7.54978995489188216e-8
    sq = rest * rest
    sine = rest + rest * sq * (
        -1.6666654611e-1 + sq * (8.3321608736e-3 + sq * -1.9515295891e-4)
    )
    cosine = 1.0 + sq * (
        -0.5 + sq * (4.166664568298827e-2 + sq * (-1.388731625493765e-3 + sq * 2.443315711809948e-5))
    )
    quadrant = turns.astype(jnp.int32)
    odd = (quadrant & 1) != 0
    cos_out = jnp.where(odd, sine, cosine)
    sin_out = jnp.where(odd, cosine, sine)
    cos_out = jnp.where(((quadrant + 1) & 2) != 0, -cos_out, cos_out)
    sin_out = jnp.where((quadrant & 2) != 0, -sin_out, sin_out)
    return cos_out, sin_out


def shell_sums(occupation, modes_x, modes_y, modes_z, limit):
    base = (modes_x[:, None] ** 2 + modes_y[None, :] ** 2) * SHELLS
    row_shell = jnp.minimum(base // limit, SHELLS - 1).reshape(-1)
    row_rest = (base % limit).reshape(-1)
    col = modes_z**2 * SHELLS
    col_shell = col // limit
    col_rest = col % limit
    flat = occupation.reshape(row_rest.shape[0], -1)
    carry = row_rest[:, None] + col_rest[None, :] >= limit
    zero = jnp.float32(0.0)
    both = jnp.concatenate([jnp.where(carry, zero, flat), jnp.where(carry, flat, zero)], axis=-1)
    shell_ids = jnp.arange(SHELLS, dtype=jnp.int32)
    hits = (row_shell[None, :] == shell_ids[:, None]).astype(jnp.float32)
    sums = jnp.einsum("sr,rc->sc", hits, both, precision=lax.Precision.HIGHEST)
    offset = jnp.concatenate([col_shell, col_shell + 1])
    shell = jnp.minimum(shell_ids[:, None] + offset[None, :], SHELLS - 1)
    picked = jnp.where(shell[None] == shell_ids[:, None, None], sums[None], zero)
    return jnp.sum(picked, axis=(1, 2))


def shards(psi_modes, noise, mask):
    grid_rank = lax.axis_index("grid")
    ranks = lax.axis_size("grid")
    extent_x = mask.shape[0]
    extent_y = noise.shape[3]
    extent_z = mask.shape[2]
    rows_local = mask.shape[1]
    planes_local = noise.shape[2]
    quarter = extent_z // 4
    chunks = max_chunks
    while planes_local % chunks:
        chunks -= 1
    depth = planes_local // chunks

    def select_cols(values):
        return jnp.concatenate([values[..., :quarter], values[..., extent_z - quarter :]], axis=-1)

    index_x, index_y, all_cols = lax.optimization_barrier(
        tuple(jnp.arange(extent, dtype=jnp.int32) for extent in (extent_x, extent_y, extent_z))
    )
    column_ids = select_cols(all_cols)
    modes_x = signed_of(index_x, extent_x)
    modes_y_all = signed_of(index_y, extent_y)
    modes_y = signed_of(grid_rank * rows_local + jnp.arange(rows_local, dtype=jnp.int32), extent_y)
    modes_z = signed_of(column_ids, extent_z)
    fac_x = axis_factor(modes_x, extent_x)
    fac_y = axis_factor(modes_y_all, extent_y)
    fac_z = axis_factor(modes_z, extent_z)
    inverse_x = block_table(scaled(dft_table(index_x, index_x, extent_x, 1.0), fac_x, 1))
    inverse_y = block_table(scaled(dft_table(index_y, index_y, extent_y, 1.0), fac_y, 1))
    inverse_z = block_table(scaled(dft_table(all_cols, column_ids, extent_z, 1.0), fac_z, 1))
    forward_x = block_table(scaled(dft_table(index_x, index_x, extent_x, -1.0), fac_x, 0))
    forward_y = block_table(scaled(dft_table(index_y, index_y, extent_y, -1.0), fac_y, 0))
    forward_z = block_table(scaled(dft_table(column_ids, all_cols, extent_z, -1.0), fac_z, 0))
    inverse_x = inverse_x.reshape(2, ranks, chunks, depth, 2, extent_x)
    inverse_y = inverse_y.reshape(2, extent_y, 2, ranks, rows_local)
    forward_y = forward_y.reshape(2, ranks, rows_local, 2, extent_y)
    forward_x = forward_x.reshape(2, extent_x, 2, ranks, chunks, depth)

    kept = select_cols(mask).astype(jnp.float32)
    start = select_cols(psi_modes) * kept
    pos_x = (grid_rank * planes_local + jnp.arange(planes_local, dtype=jnp.int32)).astype(
        jnp.float32
    )
    pos_x = (pos_x + 0.5) / extent_x - 0.5
    pos_y = (index_y.astype(jnp.float32) + 0.5) / extent_y - 0.5
    pos_z = (all_cols.astype(jnp.float32) + 0.5) / extent_z - 0.5

    def exchange(values):
        return lax.all_to_all(values, "grid", split_axis=2, concat_axis=2, tiled=True)

    arrived = [
        exchange(contract("dgpcx,tcxyz->tdgpyz", inverse_x[:, :, chunk], start))
        for chunk in range(chunks)
    ]
    final = None
    for chunk in range(chunks):
        low = chunk * depth
        spaced = contract("ekdsy,tdspyz->tepkz", inverse_y, arrived[chunk])
        field = contract("ekdz,tdpyz->tepyk", inverse_z, spaced)
        field_real, field_imag = field[:, 0], field[:, 1]
        potential = trap_strength * (
            pos_x[low : low + depth, None, None] ** 2
            + pos_y[None, :, None] ** 2
            + pos_z[None, None, :] ** 2
        )
        density = field_real * field_real + field_imag * field_imag
        energy = potential + coupling * density - chem_potential
        decay = jnp.exp(-damping * energy * time_step)
        cosine, sine = cos_sin(jnp.minimum(energy * time_step, 4096.0))
        evo_real = decay * cosine
        evo_imag = -decay * sine
        kick = noise_amp * noise[:, :, low : low + depth]
        moved = jnp.stack(
            [
                field_real * evo_real - field_imag * evo_imag + kick[:, 0],
                field_real * evo_imag + field_imag * evo_real + kick[:, 1],
            ],
            axis=1,
        )
        partial_fwd = contract("ekdz,tdpyz->tepyk", forward_z, moved)
        partial_fwd = contract("egkdy,tdpyz->tegpkz", forward_y, partial_fwd)
        returned = exchange(partial_fwd)
        piece = contract("ekdsp,tdspyz->tekyz", forward_x[:, :, :, :, chunk], returned)
        final = piece if final is None else final + piece
    out = final * kept
    occupation = jnp.sum(out * out, axis=(0, 1))
    local_hist = shell_sums(occupation, modes_x, modes_y, modes_z, 2 * quarter * quarter)
    total_hist = lax.psum(local_hist, ("traj", "grid"))
    traj_count = psi_modes.shape[0] * lax.axis_size("traj")
    momentum_hist = total_hist * (SHELLS / (traj_count * extent_x * extent_y * extent_z))
    filler = jnp.zeros(out.shape[:-1] + (extent_z - 2 * quarter,), jnp.float32)
    psi_next = jnp.concatenate([out[..., :quarter], filler, out[..., quarter:]], axis=-1)
    return (psi_next, momentum_hist)


def solution(mesh):
    placed = (
        P("traj", None, None, "grid", None),
        P("traj", None, "grid", None, None),
        P(None, "grid", None),
    )
    return jax.shard_map(
        shards,
        mesh=mesh,
        in_specs=placed,
        out_specs=(P("traj", None, None, "grid", None), P()),
        check_vma=False,
    )
```
